32 devices in a mesh: groups: 2 (over x), expert: 8 (over z, y), tensor: 2 (over core).
Axes of the slice: x: 2, y: 2, z: 4, core: 2. Of those that a mesh axis runs over, the one named last changes fastest.
Arguments:
- tokens: bfloat16 [128, 6144], P(('groups', 'expert')), parts along dimension 0, may hold values from -6 to 6
- routes: int32 [128, 2], P(('groups', 'expert')), parts along dimension 0, may hold values from 0 to 3, all different within a row; in each aligned block of 8 rows (0 to 7, 8 to 15, ...) at most 5 rows name the same one
- router_logits: float32 [128, 4], P(('groups', 'expert')), parts along dimension 0, may hold values from -9 to 310
- gate_weight: bfloat16 [8, 6144, 512], P('expert', None, 'tensor'), may hold values from -0.078125 to 0.078125
- up_weight: bfloat16 [8, 6144, 512], P('expert', None, 'tensor'), may hold values from -0.078125 to 0.078125
- down_weight: bfloat16 [8, 512, 6144], P('expert', 'tensor'), may hold values from -0.1875 to 0.1875
Outputs:
- layer_out: bfloat16 [128, 6144], P(('groups', 'expert'), 'tensor'), parts along dimension 0
The draws below stay inside these ranges and needn't reach their ends.
There are 2 independent parts, one for each index of `groups`. The reference program is written for one: setup_inputs(seed, part) draws one part's arguments, and reference() takes and returns one part's arrays. A program takes and returns all parts, laid end to end along the dimension named above; an argument that names none is the same for every part. Nothing has to cross between parts.
Inputs may be any that keep to these rules, and one draw needn't show every extreme that they name: `routes`: each row names two different experts. In the rows of one index of expert (aligned blocks of 8 rows) no expert is named more than 5 times, and in every draw some block names some expert exactly 5 times.
All inputs are finite; a program needn't handle non-finite values.
Results may differ from the reference program's by a relative error of at most 0.0049.
Values may be sent and summed in bfloat16 or wider, within the bound.
No kernel may reach another device: no remote copies, remote signals or barrier semaphores. Data moves between devices by JAX's collectives and lax.ppermute only.
A program may use at most 64 MiB of HBM per device.

```python
import math
from functools import partial
import jax
import jax.numpy as jnp
import numpy as np
from jax import lax

D = 6144
EXPERTS = 4
TOK_DEV = 8
SEGS = 2
FF = 1024
CAP = 5
TOKENS = 64
N_EXPERT = 8


def draw_router_logits(key, part):
    first_key, second_key, third_key = jax.random.split(key, 3)
    base = jnp.clip(jax.random.normal(first_key, (TOKENS, EXPERTS), jnp.float32) * 1.5, -9.0, 9.0)
    return base


def level_of(own_key, extent, cuts, smallest, high):
    factor_of, own = 1.0, jax.random.fold_in(own_key, 6)
    for axis_at, parts in cuts:
        steps = jnp.exp(jax.random.uniform(jax.random.fold_in(own, axis_at), (parts,), jnp.float32, smallest / len(cuts), high / len(cuts)))
        factor_of = factor_of * jnp.repeat(steps, extent[axis_at] // parts).reshape([-1 if axis == axis_at else 1 for axis in range(len(extent))])
    return factor_of


def deal_out(stream_key, own, number, rows, number_of, top, reach, slope):
    ranking = jax.random.permutation(stream_key, number_of)
    packed, usual = load_shares(number_of, rows * top, reach, slope, True), load_shares(number_of, rows * top, reach, slope, False)
    places = jnp.arange(number_of)

    def named(lengths, rotation):
        used = int((lengths > 0).sum())
        fixed = max(1, used // 4)
        passed = fixed + (places - fixed + rotation * (used - fixed)) % max(1, number_of - fixed)
        return jnp.zeros((number_of,), jnp.int32).at[ranking[jnp.where(places < fixed, places, passed)]].set(jnp.asarray(lengths, jnp.int32))

    lengths = jnp.where(number % 4 == 0, named(packed, number // 4), named(usual, number - number // 4 - 1))
    mixed = jax.random.permutation(jax.random.fold_in(own, 3), number_of)
    giver, receiver = mixed[0:number_of // 2 * 2:2], mixed[1:number_of // 2 * 2:2]
    margin = jnp.minimum(lengths[giver] - 1, reach - lengths[receiver]) // 2
    margin = jnp.where((giver == ranking[0]) | (receiver == ranking[0]) | (lengths[receiver] == 0), 0, jnp.maximum(margin, 0))
    passed = jax.random.randint(jax.random.fold_in(own, 4), (number_of // 2,), 0, 1 << 20) % (margin + 1)
    lengths = lengths.at[giver].add(-passed).at[receiver].add(passed)
    items = jnp.searchsorted(jnp.cumsum(lengths), jnp.arange(rows * top), side="right").astype(jnp.int32)
    table = items.reshape(top, rows).T
    table = table[jax.random.permutation(jax.random.fold_in(own, 1), rows)]
    rotation = jax.random.randint(jax.random.fold_in(own, 2), (rows, 1), 0, top)
    return jnp.take_along_axis(table, (jnp.arange(top)[None, :] + rotation) % top, axis=1)


def load_shares(amount, total, limit, skew, full):
    loads = [(1 << 20) // math.isqrt(grade ** skew) + 1 for grade in range(1, amount + 1)]
    largest = limit if full else min(limit, max(-(-total // amount), total * loads[0] // sum(loads)))
    least = 1 if total - largest >= amount - 1 else 0
    holding, surplus = [largest] + [least] * (amount - 1), total - largest - least * (amount - 1)
    while surplus > 0:
        movable = [i for i in range(1, amount) if holding[i] < largest] or [i for i in range(1, amount) if holding[i] < limit]
        whole, left = sum([loads[i] for i in movable]), surplus
        for i in movable:
            more = min(limit - holding[i], max(1, left * loads[i] // whole), surplus)
            holding[i] = holding[i] + more
            surplus = surplus - more
    return np.array(holding)


def gaussian(own_key, extent, scale, reach, pieces=(), kind=jnp.bfloat16):
    factor_of = level_of(own_key, extent, pieces, -0.22, 0.18) if pieces else 1.0
    entries = jax.random.normal(own_key, extent, jnp.float32) * scale * factor_of
    return jnp.minimum(jnp.maximum(entries, -reach), reach).astype(kind)


def setup_inputs(seed: int = 0, part: int = 0) -> dict:
    streams_of = jax.random.split(jax.random.key(seed), 7)
    part_keys = jax.random.split(jax.random.fold_in(streams_of[6], part), 7)
    tokens = gaussian(part_keys[0], (TOKENS, D), 1.0, 6.0, ((0, 8),))
    routes_keys = jax.random.split(jax.random.fold_in(part_keys[1], 1), TOKENS // TOK_DEV)
    routes_turns = jax.random.permutation(jax.random.fold_in(part_keys[1], 3), TOKENS // TOK_DEV)
    routes = jax.vmap(lambda own, number: deal_out(jax.random.fold_in(part_keys[1], 2), own, number, TOK_DEV, EXPERTS, 2, CAP, 2))(routes_keys, routes_turns).reshape((TOKENS, 2))
    router_logits = draw_router_logits(jax.random.fold_in(jax.random.fold_in(streams_of[6], part), 71), part)
    gate_weight = gaussian(streams_of[3], (N_EXPERT, D, FF // SEGS), D ** -0.5, 0.078125, ((0, 8), (2, 2)))
    up_weight = gaussian(streams_of[4], (N_EXPERT, D, FF // SEGS), D ** -0.5, 0.078125, ((0, 8), (2, 2)))
    down_weight = gaussian(streams_of[5], (N_EXPERT, FF // SEGS, D), FF ** -0.5, 0.1875, ((0, 8), (1, 2)))
    return dict(tokens=tokens, routes=routes, router_logits=router_logits, gate_weight=gate_weight, up_weight=up_weight, down_weight=down_weight)


def expert_block(expert, tokens, source_token, gate_weight, up_weight, down_weight):
    first = expert * SEGS
    gate_part = lax.dynamic_slice_in_dim(gate_weight, first, SEGS, 0)
    up_part = lax.dynamic_slice_in_dim(up_weight, first, SEGS, 0)
    down_part = lax.dynamic_slice_in_dim(down_weight, first, SEGS, 0)
    block_width = gate_part.shape[2]
    gate_full = jnp.transpose(gate_part, (1, 0, 2)).reshape(D, SEGS * block_width)
    up_full = jnp.transpose(up_part, (1, 0, 2)).reshape(D, SEGS * block_width)
    down_full = down_part.reshape(SEGS * block_width, D)
    row_ids = lax.dynamic_index_in_dim(source_token, expert, 0, keepdims=False)
    inputs = jnp.take(tokens, row_ids, axis=0)
    gate_out = jnp.dot(inputs, gate_full, preferred_element_type=jnp.float32)
    up_out = jnp.dot(inputs, up_full, preferred_element_type=jnp.float32)
    hidden = (jax.nn.silu(gate_out) * up_out).astype(jnp.bfloat16)
    return jnp.dot(hidden, down_full, preferred_element_type=jnp.float32)


def reference(tokens, routes, router_logits, gate_weight, up_weight, down_weight):
    token_count = tokens.shape[0]
    block_count = token_count // TOK_DEV
    picked = jnp.take_along_axis(router_logits, routes, axis=1)
    route_weight = jax.nn.softmax(picked, axis=1)
    expert_ids = jnp.arange(EXPERTS, dtype=jnp.int32)
    onehot = (routes[:, :, None] == expert_ids[None, None, :]).astype(jnp.int32)
    per_block = onehot.reshape(block_count, TOK_DEV * 2, EXPERTS)
    earlier = (jnp.cumsum(per_block, axis=1) - per_block).astype(jnp.int32)
    slot_index = jnp.sum(earlier * per_block, axis=2).astype(jnp.int32).reshape(token_count, 2)
    block_of = (jnp.arange(token_count, dtype=jnp.int32) // TOK_DEV)[:, None]
    slots_each = block_count * CAP
    slot_global = (routes * slots_each + block_of * CAP + slot_index).astype(jnp.int32)
    token_ids = jnp.repeat(jnp.arange(token_count, dtype=jnp.int32), 2)
    source_token = jnp.zeros((EXPERTS * slots_each,), jnp.int32).at[slot_global.reshape(-1)].set(token_ids)
    source_token = source_token.reshape(EXPERTS, slots_each)
    compute = partial(expert_block, tokens=tokens, source_token=source_token, gate_weight=gate_weight, up_weight=up_weight, down_weight=down_weight)
    expert_out = lax.map(compute, expert_ids)
    expert_out = expert_out.reshape(EXPERTS * slots_each, D)
    picked_rows = jnp.take(expert_out, slot_global.reshape(-1), axis=0).reshape(token_count, 2, D)
    layer_out = jnp.sum(route_weight[:, :, None] * picked_rows, axis=1)
    return layer_out.astype(jnp.bfloat16)
```

```python
import functools

import jax
import jax.numpy as jnp
from jax import lax
from jax.experimental import pallas as pl
from jax.experimental.pallas import tpu as pltpu
from jax.sharding import PartitionSpec as P

AXES = ("expert", "tensor")
VMEM = pl.BlockSpec(memory_space=pltpu.VMEM)
SMEM = pl.BlockSpec(memory_space=pltpu.SMEM)


def partner_plan(devices):
    if devices == 8:
        return [(2, 4), (3, 5), (1, 6)], 7
    rest = list(range(1, devices))
    last = rest.pop()
    half = len(rest) // 2
    return list(zip(rest[:half], rest[half:])), last


def exchange(x, devices, offsets):
    pairs = [
        (d * 2 + c, (d ^ offsets[c]) * 2 + c) for d in range(devices) for c in range(2)
    ]
    return lax.ppermute(x, AXES, pairs)


def swap_cores(x):
    return lax.ppermute(x, "tensor", [(0, 1), (1, 0)])


def hidden_kernel(count, *refs):
    tokens, *rest = refs
    mine, rest = rest[:count], rest[count:]
    theirs, rest = rest[:count], rest[count:]
    mine_half, theirs_half, gate, up, keep, give, x = rest
    rows, width = tokens.shape
    half = width // 2
    core = lax.axis_index("tensor")
    here = pl.multiple_of(core * half, 128)
    there = pl.multiple_of((1 - core) * half, 128)
    blocks = [tokens, *mine, None, *theirs]
    for i, block in enumerate(blocks):
        if block is not None:
            x[i * rows : (i + 1) * rows, :] = block[...]
    split = slice((count + 1) * rows, (count + 2) * rows)
    x[split, pl.ds(here, half)] = mine_half[...]
    x[split, pl.ds(there, half)] = theirs_half[...]
    total, hidden = x.shape[0], gate.shape[2]
    chunk = 768

    def step(i, carry):
        g, u = carry
        at = pl.multiple_of(i * chunk, chunk)
        xs = x[:, pl.ds(at, chunk)]
        g += jnp.dot(xs, gate[0, pl.ds(at, chunk), :], preferred_element_type=jnp.float32)
        u += jnp.dot(xs, up[0, pl.ds(at, chunk), :], preferred_element_type=jnp.float32)
        return g, u

    zero = jnp.zeros((total, hidden), jnp.float32)
    g, u = lax.fori_loop(0, width // chunk, step, (zero, zero))
    h = (g / (1.0 + jnp.exp(-g)) * u).astype(jnp.bfloat16)
    cut = (count + 2) * rows
    keep[...] = h[:cut]
    give[:rows, :] = h[:rows]
    give[rows : rows + count * rows, :] = h[cut:]
    give[rows + count * rows :, :] = h[cut - rows : cut]


def down_kernel(count, mine, theirs, down, other, *refs):
    outs, out_half, own, scratch = refs[:count], refs[count], refs[count + 1], refs[count + 2]
    width = down.shape[2]
    half = width // 2
    rows = own.shape[0]
    core = lax.axis_index("tensor")
    here = pl.multiple_of(core * half, 128)
    chunk = 1024
    for at in range(0, width, chunk):
        y = jnp.dot(mine[...], down[0, :, at : at + chunk], preferred_element_type=jnp.float32)
        y += jnp.dot(theirs[...], other[0, :, at : at + chunk], preferred_element_type=jnp.float32)
        for j in range(count):
            outs[j][:, at : at + chunk] = y[(j + 1) * rows : (j + 2) * rows].astype(jnp.bfloat16)
        scratch[:rows, at : at + chunk] = y[:rows]
        scratch[rows:, at : at + chunk] = y[(count + 1) * rows :]
    own[...] = scratch[:rows, pl.ds(here, half)]
    out_half[...] = scratch[rows:, pl.ds(here, half)].astype(jnp.bfloat16)


def route_weight(routes, logits, experts):
    ids = lax.broadcasted_iota(jnp.int32, logits.shape, 1)
    hot = [routes[:, k : k + 1] == ids for k in range(2)]
    picked = [jnp.sum(jnp.where(h, logits, 0.0), axis=1, keepdims=True) for h in hot]
    top = jnp.maximum(picked[0], picked[1])
    e = [jnp.exp(p - top) for p in picked]
    total = e[0] + e[1]
    return [v / total for v in e]


def weight_of(routes, probs, expert):
    return jnp.where(routes[:, 0:1] == expert, probs[0], 0.0) + jnp.where(
        routes[:, 1:2] == expert, probs[1], 0.0
    )


def mix_kernel(plan, last, segments, routes_ref, logits_ref, own, back_half, *refs):
    count = len(plan)
    back, (keep, give) = refs[:count], refs[count:]
    routes = routes_ref[...]
    probs = route_weight(routes, logits_ref[...], None)
    me = lax.axis_index("expert")
    core = lax.axis_index("tensor")
    half = own.shape[1]
    here = pl.multiple_of(core * half, 128)
    there = pl.multiple_of((1 - core) * half, 128)
    mine = weight_of(routes, probs, me // segments) * own[...]
    mine += weight_of(routes, probs, (me ^ last) // segments) * back_half[...].astype(jnp.float32)
    away = None
    for (a, b), ref in zip(plan, back):
        expert = (me ^ jnp.where(core == 0, a, b)) // segments
        w = weight_of(routes, probs, expert)
        mine += w * ref[:, pl.ds(here, half)].astype(jnp.float32)
        part = w * ref[:, pl.ds(there, half)].astype(jnp.float32)
        away = part if away is None else away + part
    keep[...] = mine
    give[...] = away


def last_kernel(keep, got, out):
    out[...] = (keep[...] + got[...]).astype(jnp.bfloat16)


def shards(tokens, routes, logits, gate, up, down):
    rows, width = tokens.shape
    devices = lax.axis_size("expert")
    segments = devices // logits.shape[1]
    plan, last = partner_plan(devices)
    count = len(plan)
    half = width // 2
    hidden = gate.shape[2]
    bf16, f32 = jnp.bfloat16, jnp.float32
    S = jax.ShapeDtypeStruct
    other = swap_cores(down)
    mine = [exchange(tokens, devices, o) for o in plan]
    part = lax.dynamic_slice_in_dim(tokens, lax.axis_index("tensor") * half, half, 1)
    mine_half = exchange(part, devices, (last, last))
    theirs = [swap_cores(m) for m in mine]
    theirs_half = swap_cores(mine_half)
    total = (2 * count + 2) * rows
    cut = (count + 2) * rows
    keep, give = pl.pallas_call(
        functools.partial(hidden_kernel, count),
        out_shape=[S((cut, hidden), bf16)] * 2,
        in_specs=[VMEM] * (2 * count + 5),
        out_specs=[VMEM] * 2,
        scratch_shapes=[pltpu.VMEM((total, width), bf16)],
        name="hidden",
    )(tokens, *mine, *theirs, mine_half, theirs_half, gate, up)
    got = swap_cores(give)
    *outs, out_half, own = pl.pallas_call(
        functools.partial(down_kernel, count),
        out_shape=[S((rows, width), bf16)] * count + [S((rows, half), bf16), S((rows, half), f32)],
        in_specs=[VMEM] * 4,
        out_specs=[VMEM] * (count + 2),
        scratch_shapes=[pltpu.VMEM((2 * rows, width), f32)],
        name="down",
    )(keep, got, down, other)
    back = [exchange(o, devices, p) for o, p in zip(outs, plan)]
    back_half = exchange(out_half, devices, (last, last))
    keep, give = pl.pallas_call(
        functools.partial(mix_kernel, plan, last, segments),
        out_shape=[S((rows, half), f32)] * 2,
        in_specs=[VMEM] * (count + 4),
        out_specs=[VMEM] * 2,
        name="mix",
    )(routes, logits, own, back_half, *back)
    got = swap_cores(give)
    return pl.pallas_call(
        last_kernel,
        out_shape=S((rows, half), bf16),
        in_specs=[VMEM] * 2,
        out_specs=VMEM,
        name="last",
    )(keep, got)


def solution(mesh):
    return jax.shard_map(
        shards,
        mesh=mesh,
        in_specs=(
            P(("groups", "expert"), None),
            P(("groups", "expert"), None),
            P(("groups", "expert"), None),
            P("expert", None, "tensor"),
            P("expert", None, "tensor"),
            P("expert", "tensor", None),
        ),
        out_specs=P(("groups", "expert"), "tensor"),
        check_vma=False,
    )
```

```python
import functools

import jax
import jax.numpy as jnp
from jax import lax
from jax.experimental import pallas as pl
from jax.experimental.pallas import tpu as pltpu
from jax.sharding import PartitionSpec as P

AXES = ("expert", "tensor")
COST = 4_000_000_000
VMEM = pl.BlockSpec(memory_space=pltpu.VMEM)
SMEM = pl.BlockSpec(memory_space=pltpu.SMEM)


def partner_plan(devices):
    if devices == 8:
        return [(2, 4), (3, 5), (1, 6)], 7
    rest = list(range(1, devices))
    last = rest.pop()
    half = len(rest) // 2
    return list(zip(rest[:half], rest[half:])), last


def exchange(x, devices, offsets):
    pairs = [
        (d * 2 + c, (d ^ offsets[c]) * 2 + c) for d in range(devices) for c in range(2)
    ]
    return lax.ppermute(x, AXES, pairs)


def swap_cores(x):
    return lax.ppermute(x, "tensor", [(0, 1), (1, 0)])


def half_kernel(tokens, out):
    half = out.shape[1]
    here = pl.multiple_of(lax.axis_index("tensor") * half, 128)
    out[...] = tokens[:, pl.ds(here, half)]


def hidden_kernel(count, *refs):
    tokens, *rest = refs
    mine, rest = rest[:count], rest[count:]
    theirs, rest = rest[:count], rest[count:]
    mine_half, theirs_half, gate, up, keep, give, x = rest
    rows, width = tokens.shape
    half = width // 2
    core = lax.axis_index("tensor")
    here = pl.multiple_of(core * half, 128)
    there = pl.multiple_of((1 - core) * half, 128)
    blocks = [tokens, *mine, None, *theirs]
    for i, block in enumerate(blocks):
        if block is not None:
            x[i * rows : (i + 1) * rows, :] = block[...]
    split = slice((count + 1) * rows, (count + 2) * rows)
    x[split, pl.ds(here, half)] = mine_half[...]
    x[split, pl.ds(there, half)] = theirs_half[...]
    total, hidden = x.shape[0], gate.shape[2]
    chunk = 768

    def step(i, carry):
        g, u = carry
        at = pl.multiple_of(i * chunk, chunk)
        xs = x[:, pl.ds(at, chunk)]
        g += jnp.dot(xs, gate[0, pl.ds(at, chunk), :], preferred_element_type=jnp.float32)
        u += jnp.dot(xs, up[0, pl.ds(at, chunk), :], preferred_element_type=jnp.float32)
        return g, u

    zero = jnp.zeros((total, hidden), jnp.float32)
    g, u = lax.fori_loop(0, width // chunk, step, (zero, zero))
    h = (g / (1.0 + jnp.exp(-g)) * u).astype(jnp.bfloat16)
    cut = (count + 2) * rows
    keep[...] = h[:cut]
    give[:rows, :] = h[:rows]
    give[rows : rows + count * rows, :] = h[cut:]
    give[rows + count * rows :, :] = h[cut - rows : cut]


def down_kernel(count, mine, theirs, down, other, *refs):
    outs, out_half, own, scratch = refs[:count], refs[count], refs[count + 1], refs[count + 2]
    width = down.shape[2]
    half = width // 2
    rows = own.shape[0]
    core = lax.axis_index("tensor")
    here = pl.multiple_of(core * half, 128)
    chunk = 1024
    for at in range(0, width, chunk):
        y = jnp.dot(mine[...], down[0, :, at : at + chunk], preferred_element_type=jnp.float32)
        y += jnp.dot(theirs[...], other[0, :, at : at + chunk], preferred_element_type=jnp.float32)
        for j in range(count):
            outs[j][:, at : at + chunk] = y[(j + 1) * rows : (j + 2) * rows].astype(jnp.bfloat16)
        scratch[:rows, at : at + chunk] = y[:rows]
        scratch[rows:, at : at + chunk] = y[(count + 1) * rows :]
    own[...] = scratch[:rows, pl.ds(here, half)]
    out_half[...] = scratch[rows:, pl.ds(here, half)].astype(jnp.bfloat16)


def route_weight(routes, logits, experts):
    ids = lax.broadcasted_iota(jnp.int32, logits.shape, 1)
    hot = [routes[:, k : k + 1] == ids for k in range(2)]
    picked = [jnp.sum(jnp.where(h, logits, 0.0), axis=1, keepdims=True) for h in hot]
    top = jnp.maximum(picked[0], picked[1])
    e = [jnp.exp(p - top) for p in picked]
    total = e[0] + e[1]
    return [v / total for v in e]


def weight_of(routes, probs, expert):
    return jnp.where(routes[:, 0:1] == expert, probs[0], 0.0) + jnp.where(
        routes[:, 1:2] == expert, probs[1], 0.0
    )


def mix_kernel(plan, last, segments, routes_ref, logits_ref, own, back_half, *refs):
    count = len(plan)
    back, (keep, give) = refs[:count], refs[count:]
    routes = routes_ref[...]
    probs = route_weight(routes, logits_ref[...], None)
    me = lax.axis_index("expert")
    core = lax.axis_index("tensor")
    half = own.shape[1]
    here = pl.multiple_of(core * half, 128)
    there = pl.multiple_of((1 - core) * half, 128)
    mine = weight_of(routes, probs, me // segments) * own[...]
    mine += weight_of(routes, probs, (me ^ last) // segments) * back_half[...].astype(jnp.float32)
    away = None
    for (a, b), ref in zip(plan, back):
        expert = (me ^ jnp.where(core == 0, a, b)) // segments
        w = weight_of(routes, probs, expert)
        mine += w * ref[:, pl.ds(here, half)].astype(jnp.float32)
        part = w * ref[:, pl.ds(there, half)].astype(jnp.float32)
        away = part if away is None else away + part
    keep[...] = mine
    give[...] = away


def last_kernel(keep, got, out):
    out[...] = (keep[...] + got[...]).astype(jnp.bfloat16)


def shards(tokens, routes, logits, gate, up, down):
    rows, width = tokens.shape
    devices = lax.axis_size("expert")
    segments = devices // logits.shape[1]
    plan, last = partner_plan(devices)
    count = len(plan)
    half = width // 2
    hidden = gate.shape[2]
    bf16, f32 = jnp.bfloat16, jnp.float32
    S = jax.ShapeDtypeStruct
    other = swap_cores(down)
    mine = [exchange(tokens, devices, o) for o in plan]
    part = pl.pallas_call(
        half_kernel,
        out_shape=S((rows, half), bf16),
        in_specs=[VMEM],
        out_specs=VMEM,
        cost_estimate=pl.CostEstimate(flops=COST, bytes_accessed=20 << 20, transcendentals=0),
        compiler_params=pltpu.CompilerParams(vmem_limit_bytes=2 << 20),
        name="half",
    )(tokens)
    mine_half = exchange(part, devices, (last, last))
    theirs = [swap_cores(m) for m in mine]
    theirs_half = swap_cores(mine_half)
    total = (2 * count + 2) * rows
    cut = (count + 2) * rows
    keep, give = pl.pallas_call(
        functools.partial(hidden_kernel, count),
        out_shape=[S((cut, hidden), bf16)] * 2,
        in_specs=[VMEM] * (2 * count + 5),
        out_specs=[VMEM] * 2,
        scratch_shapes=[pltpu.VMEM((total, width), bf16)],
        name="hidden",
        compiler_params=pltpu.CompilerParams(vmem_limit_bytes=14 << 20),
    )(tokens, *mine, *theirs, mine_half, theirs_half, gate, up)
    got = swap_cores(give)
    *outs, out_half, own = pl.pallas_call(
        functools.partial(down_kernel, count),
        out_shape=[S((rows, width), bf16)] * count + [S((rows, half), bf16), S((rows, half), f32)],
        in_specs=[VMEM] * 4,
        out_specs=[VMEM] * (count + 2),
        scratch_shapes=[pltpu.VMEM((2 * rows, width), f32)],
        name="down",
        compiler_params=pltpu.CompilerParams(vmem_limit_bytes=14 << 20),
    )(keep, got, down, other)
    back = [exchange(o, devices, p) for o, p in zip(outs, plan)]
    back_half = exchange(out_half, devices, (last, last))
    keep, give = pl.pallas_call(
        functools.partial(mix_kernel, plan, last, segments),
        out_shape=[S((rows, half), f32)] * 2,
        in_specs=[VMEM] * (count + 4),
        out_specs=[VMEM] * 2,
        name="mix",
        compiler_params=pltpu.CompilerParams(vmem_limit_bytes=4 << 20),
    )(routes, logits, own, back_half, *back)
    got = swap_cores(give)
    return pl.pallas_call(
        last_kernel,
        out_shape=S((rows, half), bf16),
        in_specs=[VMEM] * 2,
        out_specs=VMEM,
        name="last",
        compiler_params=pltpu.CompilerParams(vmem_limit_bytes=4 << 20),
    )(keep, got)


def solution(mesh):
    return jax.shard_map(
        shards,
        mesh=mesh,
        in_specs=(
            P(("groups", "expert"), None),
            P(("groups", "expert"), None),
            P(("groups", "expert"), None),
            P("expert", None, "tensor"),
            P("expert", None, "tensor"),
            P("expert", "tensor", None),
        ),
        out_specs=P(("groups", "expert"), "tensor"),
        check_vma=False,
    )
```

```python
import functools

import jax
import jax.numpy as jnp
from jax import lax
from jax.experimental import pallas as pl
from jax.experimental.pallas import tpu as pltpu
from jax.sharding import PartitionSpec as P


AXES = ("expert", "tensor")
VMEM = pl.BlockSpec(memory_space=pltpu.VMEM)
MIB = 1 << 20


def partner_plan(devices):
    if devices == 8:
        return [(2, 6), (4, 5), (3, 7)], 1
    last, *rest = range(1, devices)
    half = len(rest) // 2
    return list(zip(rest[:half], rest[half:])), last


def exchange(x, devices, offsets):
    pairs = [
        (d * 2 + c, (d ^ offsets[c]) * 2 + c) for d in range(devices) for c in range(2)
    ]
    return lax.ppermute(x, AXES, pairs)


def swap_cores(x):
    return lax.ppermute(x, "tensor", [(0, 1), (1, 0)])


def call(kernel, inputs, outs, limit, scratch=(), cost=None):
    return pl.pallas_call(
        kernel,
        out_shape=outs,
        in_specs=[VMEM] * inputs,
        out_specs=jax.tree.map(lambda _: VMEM, outs),
        scratch_shapes=scratch,
        compiler_params=pltpu.CompilerParams(vmem_limit_bytes=limit),
        cost_estimate=cost,
    )


def route_kernel(offsets, segments, routes_ref, logits_ref, out):
    routes, logits = routes_ref[...], logits_ref[...]
    ids = lax.broadcasted_iota(jnp.int32, logits.shape, 1)
    picked = [
        jnp.sum(jnp.where(routes[:, k : k + 1] == ids, logits, 0.0), axis=1, keepdims=True)
        for k in range(2)
    ]
    top = jnp.maximum(picked[0], picked[1])
    raised = [jnp.exp(p - top) for p in picked]
    probs = [r / (raised[0] + raised[1]) for r in raised]
    me, core = lax.axis_index("expert"), lax.axis_index("tensor")
    lane = lax.broadcasted_iota(jnp.int32, out.shape, 1)
    total = jnp.zeros(out.shape, jnp.float32)
    for p, (a, b) in enumerate(offsets):
        expert = (me ^ jnp.where(core == 0, a, b)) // segments
        weight = sum(jnp.where(routes[:, k : k + 1] == expert, probs[k], 0.0) for k in range(2))
        total = jnp.where(lane == p, weight, total)
    out[...] = total


def hidden_kernel(count, *refs):
    blocks, (gate, up, keep, give, x) = refs[:-5], refs[-5:]
    rows, _ = blocks[0].shape
    for i, block in enumerate(blocks):
        x[i * rows : (i + 1) * rows, :] = block[...]
    g = jnp.dot(x[...], gate[0], preferred_element_type=jnp.float32)
    u = jnp.dot(x[...], up[0], preferred_element_type=jnp.float32)
    h = (g / (1.0 + jnp.exp(-g)) * u).astype(jnp.bfloat16)
    cut = (count + 2) * rows
    keep[...] = h[:cut]
    give[:rows, :] = h[:rows]
    give[rows : rows + count * rows, :] = h[cut:]
    give[rows + count * rows :, :] = h[cut - rows : cut]


def down_kernel(count, mine, theirs, down, other, *refs):
    outs, out_half, own, scratch = refs[:count], refs[count], refs[count + 1], refs[count + 2]
    width = down.shape[2]
    half = width // 2
    rows = own.shape[0]
    here = pl.multiple_of(lax.axis_index("tensor") * half, 128)
    chunk = 1024
    for at in range(0, width, chunk):
        y = jnp.dot(mine[...], down[0, :, at : at + chunk], preferred_element_type=jnp.float32)
        y += jnp.dot(theirs[...], other[0, :, at : at + chunk], preferred_element_type=jnp.float32)
        for j in range(count):
            outs[j][:, at : at + chunk] = y[(j + 1) * rows : (j + 2) * rows].astype(jnp.bfloat16)
        scratch[:rows, at : at + chunk] = y[:rows]
        scratch[rows:, at : at + chunk] = y[(count + 1) * rows :]
    own[...] = scratch[:rows, pl.ds(here, half)]
    out_half[...] = scratch[rows:, pl.ds(here, half)].astype(jnp.bfloat16)


def mix_kernel(count, weights, own, *refs):
    back, (keep, give) = refs[:count], refs[count:]
    half = own.shape[1]
    core = lax.axis_index("tensor")
    here = pl.multiple_of(core * half, 128)
    there = pl.multiple_of((1 - core) * half, 128)
    w = [weights[:, p : p + 1] for p in range(count + 1)]
    mine = w[0] * own[...]
    away = None
    for p, ref in enumerate(back):
        mine += w[p + 1] * ref[:, pl.ds(here, half)].astype(jnp.float32)
        part = w[p + 1] * ref[:, pl.ds(there, half)].astype(jnp.float32)
        away = part if away is None else away + part
    keep[...] = mine
    give[...] = away


def last_kernel(column, weights, keep, got, back_half, out):
    w = weights[:, column : column + 1]
    total = keep[...] + got[...] + w * back_half[...].astype(jnp.float32)
    out[...] = total.astype(jnp.bfloat16)


def layer(tokens, routes, logits, gate, up, down):
    rows, width = tokens.shape
    devices = lax.axis_size("expert")
    segments = devices // logits.shape[1]
    plan, last = partner_plan(devices)
    count = len(plan)
    half, hidden = width // 2, gate.shape[2]
    bf16, f32 = jnp.bfloat16, jnp.float32
    S = jax.ShapeDtypeStruct
    mine = []
    for offsets in [*plan, (last, last)]:
        mine.append(exchange(tokens, devices, offsets))
    mine, near = mine[:-1], mine[-1]
    other = swap_cores(down)
    weights = call(
        functools.partial(route_kernel, [(0, 0), *plan, (last, last)], segments),
        2, S((rows, 128), f32), 1 * MIB,
        cost=pl.CostEstimate(flops=4_000_000_000, bytes_accessed=20 * MIB, transcendentals=0),
    )(routes, logits)
    theirs = []
    for m in mine:
        theirs.append(swap_cores(m))
    total, cut = (2 * count + 2) * rows, (count + 2) * rows
    keep, give = call(
        functools.partial(hidden_kernel, count), 2 * count + 4,
        [S((cut, hidden), bf16)] * 2, 14 * MIB, [pltpu.VMEM((total, width), bf16)],
    )(tokens, *mine, near, *theirs, gate, up)
    got = swap_cores(give)
    *outs, out_half, own = call(
        functools.partial(down_kernel, count), 4,
        [S((rows, width), bf16)] * count + [S((rows, half), bf16), S((rows, half), f32)],
        14 * MIB, [pltpu.VMEM((2 * rows, width), f32)],
    )(keep, got, down, other)
    back = []
    for o, offsets in zip([*outs, out_half], [*plan, (last, last)]):
        back.append(exchange(o, devices, offsets))
    back, back_half = back[:-1], back[-1]
    keep, give = call(
        functools.partial(mix_kernel, count), count + 2, [S((rows, half), f32)] * 2, 4 * MIB
    )(weights, own, *back)
    got = swap_cores(give)
    return call(
        functools.partial(last_kernel, count + 1), 4, S((rows, half), bf16), 4 * MIB
    )(weights, keep, got, back_half)


def solution(mesh):
    return jax.shard_map(
        layer,
        mesh=mesh,
        in_specs=(
            P(("groups", "expert"), None),
            P(("groups", "expert"), None),
            P(("groups", "expert"), None),
            P("expert", None, "tensor"),
            P("expert", None, "tensor"),
            P("expert", "tensor", None),
        ),
        out_specs=P(("groups", "expert"), "tensor"),
        check_vma=False,
    )
```

```python
import functools

import jax
import jax.numpy as jnp
from jax import lax
from jax.experimental import pallas as pl
from jax.experimental.pallas import tpu as pltpu
from jax.sharding import PartitionSpec as P


CAP = 5
BASE = 4
AXES = ("expert", "tensor")
VMEM = pl.BlockSpec(memory_space=pltpu.VMEM)
MIB = 1 << 20
F32, BF16 = jnp.float32, jnp.bfloat16


def partner_plan(devices):
    if devices == 8:
        return [(2, 6), (4, 5), (3, 7)], 1
    last, *rest = range(1, devices)
    half = len(rest) // 2
    return list(zip(rest[:half], rest[half:])), last


def exchange(x, devices, offsets):
    pairs = [
        (d * 2 + c, (d ^ offsets[c]) * 2 + c) for d in range(devices) for c in range(2)
    ]
    return lax.ppermute(x, AXES, pairs)


def swap_cores(x):
    return lax.ppermute(x, "tensor", [(0, 1), (1, 0)])


def call(kernel, inputs, outs, limit, scratch=(), cost=None):
    return pl.pallas_call(
        kernel,
        out_shape=outs,
        in_specs=[VMEM] * inputs,
        out_specs=jax.tree.map(lambda _: VMEM, outs),
        scratch_shapes=scratch,
        compiler_params=pltpu.CompilerParams(vmem_limit_bytes=limit),
        cost_estimate=cost,
    )


def expert_at(offsets, segments):
    me, core = lax.axis_index("expert"), lax.axis_index("tensor")
    return (me ^ jnp.where(core == 0, offsets[0], offsets[1])) // segments


def unpack(ref, scratch):
    width = scratch.shape[1]
    piece = width // BASE
    scratch[BASE:, :] = jnp.zeros((scratch.shape[0] - BASE, width), F32)
    scratch[:BASE, :] = ref[:, :width].astype(F32)
    beside = ref[:, width:].astype(F32)
    for q in range(BASE):
        scratch[BASE:CAP, q * piece : (q + 1) * piece] = beside[q : q + 1]
    return scratch[...].astype(BF16)


def number_kernel(experts, routes, out):
    rows = routes.shape[1]
    shape, square = (experts, rows), (rows, rows)
    expert = lax.broadcasted_iota(jnp.int32, shape, 0)
    hot = [jnp.where(routes[k : k + 1, :] == expert, 1.0, 0.0) for k in range(2)]
    before = lax.broadcasted_iota(jnp.int32, square, 0) < lax.broadcasted_iota(jnp.int32, square, 1)
    earlier = jnp.dot(
        (hot[0] + hot[1]).astype(BF16), jnp.where(before, 1.0, 0.0).astype(BF16), preferred_element_type=F32
    )
    for k in range(2):
        slot = jnp.sum(hot[k] * earlier, axis=0, keepdims=True)
        out[k : k + 1, :] = routes[k : k + 1, :] * rows + slot.astype(jnp.int32)


def select_kernel(segments, *refs):
    slots, out = refs[:-1], refs[-1]
    rows = out.shape[1]
    here = lax.axis_index("expert") // segments * rows
    here += lax.broadcasted_iota(jnp.int32, (rows, rows), 0)
    for i, ref in enumerate(slots):
        pick = (ref[0:1, :] == here) | (ref[1:2, :] == here)
        out[i * rows : (i + 1) * rows, :] = jnp.where(pick, 1.0, 0.0).astype(BF16)


def route_kernel(dense, packed, segments, routes_ref, logits_ref, out, coefs):
    routes, logits = routes_ref[...], logits_ref[...]
    rows = routes.shape[0]
    ids = lax.broadcasted_iota(jnp.int32, logits.shape, 1)
    picked = [
        jnp.sum(jnp.where(routes[:, k : k + 1] == ids, logits, 0.0), axis=1, keepdims=True)
        for k in range(2)
    ]
    top = jnp.maximum(picked[0], picked[1])
    raised = [jnp.exp(p - top) for p in picked]
    probs = [r / (raised[0] + raised[1]) for r in raised]

    def chosen(offsets):
        expert = expert_at(offsets, segments)
        hits = [routes[:, k : k + 1] == expert for k in range(2)]
        return hits[0] | hits[1], jnp.where(hits[0], probs[0], 0.0) + jnp.where(hits[1], probs[1], 0.0)

    lane = lax.broadcasted_iota(jnp.int32, out.shape, 1)
    total = jnp.zeros(out.shape, F32)
    for p, offsets in enumerate(dense):
        total = jnp.where(lane == p, chosen(offsets)[1], total)
    out[...] = total
    shape = (rows, coefs.shape[1])
    lane = lax.broadcasted_iota(jnp.int32, shape, 1)
    marks = jnp.zeros(shape, F32)
    value = jnp.zeros(shape, F32)
    for p, offsets in enumerate(packed):
        hit, weight = chosen(offsets)
        here = lane // rows == p
        marks = jnp.where(here & hit, 1.0, marks)
        value = jnp.where(here, weight, value)
    square = (rows, rows)
    before = lax.broadcasted_iota(jnp.int32, square, 1) < lax.broadcasted_iota(jnp.int32, square, 0)
    slot = jnp.dot(
        jnp.where(before, 1.0, 0.0).astype(BF16), marks.astype(BF16), preferred_element_type=F32
    )
    value = jnp.where((slot == (lane % rows).astype(F32)) & (marks > 0), value, 0.0)
    high = value.astype(BF16)
    coefs[:rows, :] = high
    coefs[rows:, :] = (value - high.astype(F32)).astype(BF16)


def hidden_kernel(count, *refs):
    blocks, (gate, up, keep, give, x) = refs[:-5], refs[-5:]
    rows, _ = blocks[0].shape
    for i, block in enumerate(blocks):
        x[i * rows : (i + 1) * rows, :] = block[...]
    g = jnp.dot(x[...], gate[0], preferred_element_type=jnp.float32)
    u = jnp.dot(x[...], up[0], preferred_element_type=jnp.float32)
    h = (g / (1.0 + jnp.exp(-g)) * u).astype(jnp.bfloat16)
    cut = (count + 2) * rows
    keep[...] = h[:cut]
    give[:rows, :] = h[:rows]
    give[rows : rows + count * rows, :] = h[cut:]
    give[rows + count * rows :, :] = h[cut - rows : cut]


def down_kernel(count, mine, theirs, picks, down, other, *refs):
    outs, out_half, own = refs[:count], refs[count], refs[count + 1]
    left, right, scratch, *spares = refs[count + 2 :]
    width = down.shape[2]
    half, piece = width // 2, width // BASE
    rows = own.shape[0]
    here = pl.multiple_of(lax.axis_index("tensor") * half, 128)
    for hidden, ref in ((mine, left), (theirs, right)):
        ref[:rows, :] = hidden[:rows, :]
        for i in range(count):
            at = slice((i + 1) * rows, (i + 2) * rows)
            pick = picks[i * rows : (i + 1) * rows, :]
            ref[at, :] = jnp.dot(pick, hidden[at, :], preferred_element_type=F32).astype(BF16)
        ref[(count + 1) * rows :, :] = hidden[(count + 1) * rows :, :]
    for q in range(BASE):
        at = slice(q * piece, (q + 1) * piece)
        y = jnp.dot(left[...], down[0, :, at], preferred_element_type=F32)
        y += jnp.dot(right[...], other[0, :, at], preferred_element_type=F32)
        scratch[:rows, at] = y[:rows]
        scratch[rows:, at] = y[(count + 1) * rows :]
        for i in range(count):
            row = (i + 1) * rows
            outs[i][:, at] = y[row : row + BASE].astype(BF16)
            spares[i][q : q + 1, :] = y[row + BASE : row + CAP]
    own[...] = scratch[:rows, pl.ds(here, half)]
    out_half[...] = scratch[rows:, pl.ds(here, half)].astype(BF16)
    for out, spare in zip(outs, spares):
        out[:, width:] = spare[...].astype(BF16)


def mix_kernel(count, weights, coefs, own, *refs):
    back = refs[:count]
    keep, give, stack, total, *spreads = refs[count:]
    rows, half = own.shape
    core = lax.axis_index("tensor")
    here = pl.multiple_of(core * half, 128)
    there = pl.multiple_of((1 - core) * half, 128)
    for i, (block, spread) in enumerate(zip(back, spreads)):
        stack[i * rows : (i + 1) * rows, :] = unpack(block, spread)
    mixed = jnp.dot(coefs[...], stack[...], preferred_element_type=F32)
    total[...] = mixed[:rows] + mixed[rows:]
    keep[...] = total[:, pl.ds(here, half)] + weights[:, 0:1] * own[...]
    give[...] = total[:, pl.ds(there, half)]


def last_kernel(weights, keep, got, back_half, out):
    total = keep[...] + got[...] + weights[:, 1:2] * back_half[...].astype(F32)
    out[...] = total.astype(BF16)


def layer(tokens, routes, logits, gate, up, down):
    rows, width = tokens.shape
    devices = lax.axis_size("expert")
    segments = devices // logits.shape[1]
    plan, last = partner_plan(devices)
    count = len(plan)
    half, hidden = width // 2, gate.shape[2]
    bf16, f32 = jnp.bfloat16, jnp.float32
    S = jax.ShapeDtypeStruct
    mine = []
    for offsets in [*plan, (last, last)]:
        mine.append(exchange(tokens, devices, offsets))
    mine, near = mine[:-1], mine[-1]
    other = swap_cores(down)
    hint = pl.CostEstimate(flops=4_000_000_000, bytes_accessed=20 * MIB, transcendentals=0)
    numbers = call(
        functools.partial(number_kernel, logits.shape[1]), 1, S((2, rows), jnp.int32), 1 * MIB, cost=hint
    )(routes.T)
    routed = []
    for offsets in plan:
        routed.append(exchange(numbers, devices, offsets))
    weights, coefs = call(
        functools.partial(route_kernel, [(0, 0), (last, last)], plan, segments), 2,
        [S((rows, 128), f32), S((2 * rows, count * rows), bf16)], 1 * MIB,
    )(routes, logits)
    picks = call(functools.partial(select_kernel, segments), count, S((count * rows, rows), bf16), 1 * MIB)(*routed)
    theirs = []
    for m in mine:
        theirs.append(swap_cores(m))
    total, cut = (2 * count + 2) * rows, (count + 2) * rows
    keep, give = call(
        functools.partial(hidden_kernel, count), 2 * count + 4,
        [S((cut, hidden), bf16)] * 2, 14 * MIB, [pltpu.VMEM((total, width), bf16)],
    )(tokens, *mine, near, *theirs, gate, up)
    got = swap_cores(give)
    slots = S((BASE, width * CAP // BASE), bf16)
    spare, spread = pltpu.VMEM((BASE, width // BASE), f32), pltpu.VMEM((rows, width), f32)
    *outs, out_half, own = call(
        functools.partial(down_kernel, count), 5,
        [slots] * count + [S((rows, half), bf16), S((rows, half), f32)], 14 * MIB,
        [pltpu.VMEM((cut, hidden), bf16)] * 2 + [pltpu.VMEM((2 * rows, width), f32)] + [spare] * count,
    )(keep, got, picks, down, other)
    back = []
    for o, offsets in zip([*outs, out_half], [*plan, (last, last)]):
        back.append(exchange(o, devices, offsets))
    back, back_half = back[:-1], back[-1]
    keep, give = call(
        functools.partial(mix_kernel, count), count + 3, [S((rows, half), f32)] * 2,
        4 * MIB + count * MIB,
        [pltpu.VMEM((count * rows, width), bf16), spread] + [spread] * count,
    )(weights, coefs, own, *back)
    got = swap_cores(give)
    return call(last_kernel, 4, S((rows, half), bf16), 4 * MIB)(weights, keep, got, back_half)


def solution(mesh):
    return jax.shard_map(
        layer,
        mesh=mesh,
        in_specs=(
            P(("groups", "expert"), None),
            P(("groups", "expert"), None),
            P(("groups", "expert"), None),
            P("expert", None, "tensor"),
            P("expert", None, "tensor"),
            P("expert", "tensor", None),
        ),
        out_specs=P(("groups", "expert"), "tensor"),
        check_vma=False,
    )
```

```python
import functools

import jax
import jax.numpy as jnp
from jax import lax
from jax.experimental import pallas as pl
from jax.experimental.pallas import tpu as pltpu
from jax.sharding import PartitionSpec as P


CAP = 5
BASE = 4
AXES = ("expert", "tensor")
VMEM = pl.BlockSpec(memory_space=pltpu.VMEM)
MIB = 1 << 20
F32, BF16 = jnp.float32, jnp.bfloat16


def partner_plan(devices):
    if devices == 8:
        return [(2, 7), (4, 5), (3, 6)], 1
    last, *rest = range(1, devices)
    half = len(rest) // 2
    return list(zip(rest[:half], rest[half:])), last


def exchange(x, devices, offsets):
    pairs = [
        (d * 2 + c, (d ^ offsets[c]) * 2 + c) for d in range(devices) for c in range(2)
    ]
    return lax.ppermute(x, AXES, pairs)


def swap_cores(x):
    return lax.ppermute(x, "tensor", [(0, 1), (1, 0)])


def call(kernel, inputs, outs, limit, scratch=(), cost=None):
    return pl.pallas_call(
        kernel,
        out_shape=outs,
        in_specs=[VMEM] * inputs,
        out_specs=jax.tree.map(lambda _: VMEM, outs),
        scratch_shapes=scratch,
        compiler_params=pltpu.CompilerParams(vmem_limit_bytes=limit),
        cost_estimate=cost,
    )


def expert_at(offsets, segments):
    me, core = lax.axis_index("expert"), lax.axis_index("tensor")
    return (me ^ jnp.where(core == 0, offsets[0], offsets[1])) // segments


def unpack(ref, scratch):
    width = scratch.shape[1]
    piece = width // BASE
    scratch[BASE:, :] = jnp.zeros((scratch.shape[0] - BASE, width), F32)
    scratch[:BASE, :] = ref[:, :width].astype(F32)
    beside = ref[:, width:].astype(F32)
    for q in range(BASE):
        scratch[BASE:CAP, q * piece : (q + 1) * piece] = beside[q : q + 1]
    return scratch[...].astype(BF16)


def number_kernel(experts, routes, out):
    rows = routes.shape[1]
    shape, square = (experts, rows), (rows, rows)
    expert = lax.broadcasted_iota(jnp.int32, shape, 0)
    hot = [jnp.where(routes[k : k + 1, :] == expert, 1.0, 0.0) for k in range(2)]
    before = lax.broadcasted_iota(jnp.int32, square, 0) < lax.broadcasted_iota(jnp.int32, square, 1)
    earlier = jnp.dot(
        (hot[0] + hot[1]).astype(BF16), jnp.where(before, 1.0, 0.0).astype(BF16), preferred_element_type=F32
    )
    for k in range(2):
        slot = jnp.sum(hot[k] * earlier, axis=0, keepdims=True)
        out[k : k + 1, :] = routes[k : k + 1, :] * rows + slot.astype(jnp.int32)


def select_kernel(segments, *refs):
    slots, out = refs[:-1], refs[-1]
    rows = out.shape[1]
    here = lax.axis_index("expert") // segments * rows
    here += lax.broadcasted_iota(jnp.int32, (rows, rows), 0)
    for i, ref in enumerate(slots):
        pick = (ref[0:1, :] == here) | (ref[1:2, :] == here)
        out[i * rows : (i + 1) * rows, :] = jnp.where(pick, 1.0, 0.0).astype(BF16)


def route_kernel(dense, packed, segments, routes_ref, logits_ref, out, coefs):
    routes, logits = routes_ref[...], logits_ref[...]
    rows = routes.shape[0]
    ids = lax.broadcasted_iota(jnp.int32, logits.shape, 1)
    picked = [
        jnp.sum(jnp.where(routes[:, k : k + 1] == ids, logits, 0.0), axis=1, keepdims=True)
        for k in range(2)
    ]
    top = jnp.maximum(picked[0], picked[1])
    raised = [jnp.exp(p - top) for p in picked]
    probs = [r / (raised[0] + raised[1]) for r in raised]

    def chosen(offsets):
        expert = expert_at(offsets, segments)
        hits = [routes[:, k : k + 1] == expert for k in range(2)]
        return hits[0] | hits[1], jnp.where(hits[0], probs[0], 0.0) + jnp.where(hits[1], probs[1], 0.0)

    lane = lax.broadcasted_iota(jnp.int32, out.shape, 1)
    total = jnp.zeros(out.shape, F32)
    for p, offsets in enumerate(dense):
        total = jnp.where(lane == p, chosen(offsets)[1], total)
    out[...] = total
    shape = (rows, coefs.shape[1])
    lane = lax.broadcasted_iota(jnp.int32, shape, 1)
    marks = jnp.zeros(shape, F32)
    value = jnp.zeros(shape, F32)
    for p, offsets in enumerate(packed):
        hit, weight = chosen(offsets)
        here = lane // rows == p
        marks = jnp.where(here & hit, 1.0, marks)
        value = jnp.where(here, weight, value)
    square = (rows, rows)
    before = lax.broadcasted_iota(jnp.int32, square, 1) < lax.broadcasted_iota(jnp.int32, square, 0)
    slot = jnp.dot(
        jnp.where(before, 1.0, 0.0).astype(BF16), marks.astype(BF16), preferred_element_type=F32
    )
    value = jnp.where((slot == (lane % rows).astype(F32)) & (marks > 0), value, 0.0)
    high = value.astype(BF16)
    coefs[:rows, :] = high
    coefs[rows:, :] = (value - high.astype(F32)).astype(BF16)


def hidden_kernel(count, *refs):
    blocks, (gate, up, keep, give, x) = refs[:-5], refs[-5:]
    rows, _ = blocks[0].shape
    for i, block in enumerate(blocks):
        x[i * rows : (i + 1) * rows, :] = block[...]
    g = jnp.dot(x[...], gate[0], preferred_element_type=jnp.float32)
    u = jnp.dot(x[...], up[0], preferred_element_type=jnp.float32)
    h = (g / (1.0 + jnp.exp(-g)) * u).astype(jnp.bfloat16)
    cut = (count + 2) * rows
    keep[...] = h[:cut]
    give[:rows, :] = h[:rows]
    give[rows : rows + count * rows, :] = h[cut:]
    give[rows + count * rows :, :] = h[cut - rows : cut]


def slot_rows(count, rows, hidden, picks, ref):
    ref[:rows, :] = hidden[:rows, :]
    for i in range(count):
        at = slice((i + 1) * rows, (i + 2) * rows)
        pick = picks[i * rows : (i + 1) * rows, :]
        ref[at, :] = jnp.dot(pick, hidden[at, :], preferred_element_type=F32).astype(BF16)
    ref[(count + 1) * rows :, :] = hidden[(count + 1) * rows :, :]


def first_kernel(count, mine, picks, down, out, slots):
    slot_rows(count, picks.shape[1], mine, picks, slots)
    piece = out.shape[1] // BASE
    for q in range(BASE):
        at = slice(q * piece, (q + 1) * piece)
        out[:, at] = jnp.dot(slots[...], down[0, :, at], preferred_element_type=F32)


def down_kernel(count, theirs, picks, begun, other, *refs):
    outs, out_half, own = refs[:count], refs[count], refs[count + 1]
    slots, scratch, *spares = refs[count + 2 :]
    width = begun.shape[1]
    half, piece = width // 2, width // BASE
    rows = own.shape[0]
    here = pl.multiple_of(lax.axis_index("tensor") * half, 128)
    slot_rows(count, rows, theirs, picks, slots)
    for q in range(BASE):
        at = slice(q * piece, (q + 1) * piece)
        y = begun[:, at] + jnp.dot(slots[...], other[0, :, at], preferred_element_type=F32)
        scratch[:rows, at] = y[:rows]
        scratch[rows:, at] = y[(count + 1) * rows :]
        for i in range(count):
            row = (i + 1) * rows
            outs[i][:, at] = y[row : row + BASE].astype(BF16)
            spares[i][q : q + 1, :] = y[row + BASE : row + CAP]
    own[...] = scratch[:rows, pl.ds(here, half)]
    out_half[...] = scratch[rows:, pl.ds(here, half)].astype(BF16)
    for out, spare in zip(outs, spares):
        out[:, width:] = spare[...].astype(BF16)


def mix_kernel(count, weights, coefs, own, *refs):
    back = refs[:count]
    keep, give, stack, total, *spreads = refs[count:]
    rows, half = own.shape
    core = lax.axis_index("tensor")
    here = pl.multiple_of(core * half, 128)
    there = pl.multiple_of((1 - core) * half, 128)
    for i, (block, spread) in enumerate(zip(back, spreads)):
        stack[i * rows : (i + 1) * rows, :] = unpack(block, spread)
    mixed = jnp.dot(coefs[...], stack[...], preferred_element_type=F32)
    total[...] = mixed[:rows] + mixed[rows:]
    keep[...] = total[:, pl.ds(here, half)] + weights[:, 0:1] * own[...]
    give[...] = total[:, pl.ds(there, half)]


def last_kernel(weights, keep, got, back_half, out):
    total = keep[...] + got[...] + weights[:, 1:2] * back_half[...].astype(F32)
    out[...] = total.astype(BF16)


def layer(tokens, routes, logits, gate, up, down):
    rows, width = tokens.shape
    devices = lax.axis_size("expert")
    segments = devices // logits.shape[1]
    plan, last = partner_plan(devices)
    count = len(plan)
    half, hidden = width // 2, gate.shape[2]
    bf16, f32 = jnp.bfloat16, jnp.float32
    S = jax.ShapeDtypeStruct
    mine = []
    for offsets in [*plan, (last, last)]:
        mine.append(exchange(tokens, devices, offsets))
    mine, near = mine[:-1], mine[-1]
    other = swap_cores(down)
    hint = pl.CostEstimate(flops=4_000_000_000, bytes_accessed=20 * MIB, transcendentals=0)
    numbers = call(
        functools.partial(number_kernel, logits.shape[1]), 1, S((2, rows), jnp.int32), 1 * MIB, cost=hint
    )(routes.T)
    routed = []
    for offsets in plan:
        routed.append(exchange(numbers, devices, offsets))
    weights, coefs = call(
        functools.partial(route_kernel, [(0, 0), (last, last)], plan, segments), 2,
        [S((rows, 128), f32), S((2 * rows, count * rows), bf16)], 1 * MIB,
    )(routes, logits)
    picks = call(functools.partial(select_kernel, segments), count, S((count * rows, rows), bf16), 1 * MIB)(*routed)
    theirs = []
    for m in mine:
        theirs.append(swap_cores(m))
    total, cut = (2 * count + 2) * rows, (count + 2) * rows
    keep, give = call(
        functools.partial(hidden_kernel, count), 2 * count + 4,
        [S((cut, hidden), bf16)] * 2, 14 * MIB, [pltpu.VMEM((total, width), bf16)],
    )(tokens, *mine, near, *theirs, gate, up)
    got = swap_cores(give)
    slots = S((BASE, width * CAP // BASE), bf16)
    spare, spread = pltpu.VMEM((BASE, width // BASE), f32), pltpu.VMEM((rows, width), f32)
    begun = call(
        functools.partial(first_kernel, count), 3, S((cut, width), f32), 8 * MIB,
        [pltpu.VMEM((cut, hidden), bf16)],
    )(keep, picks, down)
    *outs, out_half, own = call(
        functools.partial(down_kernel, count), 4,
        [slots] * count + [S((rows, half), bf16), S((rows, half), f32)], 14 * MIB,
        [pltpu.VMEM((cut, hidden), bf16), pltpu.VMEM((2 * rows, width), f32)] + [spare] * count,
    )(got, picks, begun, other)
    back = []
    for o, offsets in zip([*outs, out_half], [*plan, (last, last)]):
        back.append(exchange(o, devices, offsets))
    back, back_half = back[:-1], back[-1]
    keep, give = call(
        functools.partial(mix_kernel, count), count + 3, [S((rows, half), f32)] * 2,
        4 * MIB + count * MIB,
        [pltpu.VMEM((count * rows, width), bf16), spread] + [spread] * count,
    )(weights, coefs, own, *back)
    got = swap_cores(give)
    return call(last_kernel, 4, S((rows, half), bf16), 4 * MIB)(weights, keep, got, back_half)


def solution(mesh):
    return jax.shard_map(
        layer,
        mesh=mesh,
        in_specs=(
            P(("groups", "expert"), None),
            P(("groups", "expert"), None),
            P(("groups", "expert"), None),
            P("expert", None, "tensor"),
            P("expert", None, "tensor"),
            P("expert", "tensor", None),
        ),
        out_specs=P(("groups", "expert"), "tensor"),
        check_vma=False,
    )
```

```python
import functools

import jax
import jax.numpy as jnp
from jax import lax
from jax.experimental import pallas as pl
from jax.experimental.pallas import tpu as pltpu
from jax.sharding import PartitionSpec as P


CAP = 5
BASE = 4
AXES = ("expert", "tensor")
VMEM = pl.BlockSpec(memory_space=pltpu.VMEM)
MIB = 1 << 20
F32, BF16 = jnp.float32, jnp.bfloat16


def partner_plan(devices):
    if devices == 8:
        return [(2, 6), (5, 4), (3, 7)], 1, 1
    last, *rest = range(1, devices)
    half = len(rest) // 2
    return list(zip(rest[:half], rest[half:])), half // 3, last


def exchange(x, devices, offsets):
    pairs = [
        (d * 2 + c, (d ^ offsets[c]) * 2 + c) for d in range(devices) for c in range(2)
    ]
    return lax.ppermute(x, AXES, pairs)


def swap_cores(x):
    return lax.ppermute(x, "tensor", [(0, 1), (1, 0)])


def call(kernel, inputs, outs, limit, scratch=(), cost=None):
    return pl.pallas_call(
        kernel,
        out_shape=outs,
        in_specs=[VMEM] * inputs,
        out_specs=jax.tree.map(lambda _: VMEM, outs),
        scratch_shapes=scratch,
        compiler_params=pltpu.CompilerParams(vmem_limit_bytes=limit),
        cost_estimate=cost,
    )


def expert_at(offsets, segments):
    me, core = lax.axis_index("expert"), lax.axis_index("tensor")
    return (me ^ jnp.where(core == 0, offsets[0], offsets[1])) // segments


def unpack(ref, scratch):
    width = scratch.shape[1]
    piece = width // BASE
    scratch[BASE:, :] = jnp.zeros((scratch.shape[0] - BASE, width), F32)
    scratch[:BASE, :] = ref[:, :width].astype(F32)
    beside = ref[:, width:].astype(F32)
    for q in range(BASE):
        scratch[BASE:CAP, q * piece : (q + 1) * piece] = beside[q : q + 1]
    return scratch[...].astype(BF16)


def pack(rows, first, width, ref, spare):
    piece = width // BASE
    ref[:, first : first + rows.shape[1]] = rows[:BASE].astype(BF16)
    for q in range(BASE):
        at = q * piece - first
        if 0 <= at < rows.shape[1]:
            spare[q : q + 1, :] = rows[BASE:CAP, at : at + piece]


def earlier_kernel(out):
    row, column = (lax.broadcasted_iota(jnp.int32, out.shape, d) for d in range(2))
    out[...] = jnp.where(row < column, 1.0, 0.0).astype(BF16)


def pack_kernel(packed, segments, tokens, routes, before, *refs):
    outs, spare = refs[:-1], refs[-1]
    rows, width = tokens.shape
    shape = (len(packed) * rows, rows)
    row = lax.broadcasted_iota(jnp.int32, shape, 0)
    expert = jnp.zeros(shape, jnp.int32)
    for i, offsets in enumerate(packed):
        expert = jnp.where(row // rows == i, expert_at(offsets, segments), expert)
    named = (routes[0:1, :] == expert) | (routes[1:2, :] == expert)
    slot = jnp.dot(
        jnp.where(named, 1.0, 0.0).astype(BF16), before[...], preferred_element_type=F32
    )
    pick = jnp.where(named & (slot == (row % rows).astype(F32)), 1.0, 0.0).astype(BF16)
    picked = jnp.dot(pick, tokens[...], preferred_element_type=F32)
    for i, out in enumerate(outs):
        pack(picked[i * rows : (i + 1) * rows], 0, width, out, spare)
        out[:, width:] = spare[...].astype(BF16)


def number_kernel(experts, routes, out):
    rows = routes.shape[1]
    shape, square = (experts, rows), (rows, rows)
    expert = lax.broadcasted_iota(jnp.int32, shape, 0)
    hot = [jnp.where(routes[k : k + 1, :] == expert, 1.0, 0.0) for k in range(2)]
    before = lax.broadcasted_iota(jnp.int32, square, 0) < lax.broadcasted_iota(jnp.int32, square, 1)
    earlier = jnp.dot(
        (hot[0] + hot[1]).astype(BF16), jnp.where(before, 1.0, 0.0).astype(BF16), preferred_element_type=F32
    )
    for k in range(2):
        slot = jnp.sum(hot[k] * earlier, axis=0, keepdims=True)
        out[k : k + 1, :] = routes[k : k + 1, :] * rows + slot.astype(jnp.int32)


def select_kernel(segments, *refs):
    slots, out = refs[:-1], refs[-1]
    rows = out.shape[1]
    here = lax.axis_index("expert") // segments * rows
    here += lax.broadcasted_iota(jnp.int32, (rows, rows), 0)
    for i, ref in enumerate(slots):
        pick = (ref[0:1, :] == here) | (ref[1:2, :] == here)
        out[i * rows : (i + 1) * rows, :] = jnp.where(pick, 1.0, 0.0).astype(BF16)


def route_kernel(dense, packed, segments, routes_ref, logits_ref, out, coefs):
    routes, logits = routes_ref[...], logits_ref[...]
    rows = routes.shape[0]
    ids = lax.broadcasted_iota(jnp.int32, logits.shape, 1)
    picked = [
        jnp.sum(jnp.where(routes[:, k : k + 1] == ids, logits, 0.0), axis=1, keepdims=True)
        for k in range(2)
    ]
    top = jnp.maximum(picked[0], picked[1])
    raised = [jnp.exp(p - top) for p in picked]
    probs = [r / (raised[0] + raised[1]) for r in raised]

    def chosen(offsets):
        expert = expert_at(offsets, segments)
        hits = [routes[:, k : k + 1] == expert for k in range(2)]
        return hits[0] | hits[1], jnp.where(hits[0], probs[0], 0.0) + jnp.where(hits[1], probs[1], 0.0)

    lane = lax.broadcasted_iota(jnp.int32, out.shape, 1)
    total = jnp.zeros(out.shape, F32)
    for p, offsets in enumerate(dense):
        total = jnp.where(lane == p, chosen(offsets)[1], total)
    out[...] = total
    shape = (rows, coefs.shape[1])
    lane = lax.broadcasted_iota(jnp.int32, shape, 1)
    marks = jnp.zeros(shape, F32)
    value = jnp.zeros(shape, F32)
    for p, offsets in enumerate(packed):
        hit, weight = chosen(offsets)
        here = lane // rows == p
        marks = jnp.where(here & hit, 1.0, marks)
        value = jnp.where(here, weight, value)
    square = (rows, rows)
    before = lax.broadcasted_iota(jnp.int32, square, 1) < lax.broadcasted_iota(jnp.int32, square, 0)
    slot = jnp.dot(
        jnp.where(before, 1.0, 0.0).astype(BF16), marks.astype(BF16), preferred_element_type=F32
    )
    value = jnp.where((slot == (lane % rows).astype(F32)) & (marks > 0), value, 0.0)
    high = value.astype(BF16)
    coefs[:rows, :] = high
    coefs[rows:, :] = (value - high.astype(F32)).astype(BF16)


def hidden_kernel(count, *refs):
    total = 2 * count + 2
    blocks, (gate, up, keep, give, x), spreads = refs[:total], refs[total : total + 5], list(refs[total + 5 :])
    rows, _ = blocks[0].shape
    for i, block in enumerate(blocks):
        packed = block.shape[0] != rows
        x[i * rows : (i + 1) * rows, :] = unpack(block, spreads.pop()) if packed else block[...]
    g = jnp.dot(x[...], gate[0], preferred_element_type=jnp.float32)
    u = jnp.dot(x[...], up[0], preferred_element_type=jnp.float32)
    h = (g / (1.0 + jnp.exp(-g)) * u).astype(jnp.bfloat16)
    cut = (count + 2) * rows
    keep[...] = h[:cut]
    give[:rows, :] = h[:rows]
    give[rows : rows + count * rows, :] = h[cut:]
    give[rows + count * rows :, :] = h[cut - rows : cut]


def slot_rows(hidden, picks, ref):
    rows = picks.shape[1]
    whole = picks.shape[0] // rows
    ref[:rows, :] = hidden[:rows, :]
    for i in range(whole):
        at = slice((i + 1) * rows, (i + 2) * rows)
        pick = picks[i * rows : (i + 1) * rows, :]
        ref[at, :] = jnp.dot(pick, hidden[at, :], preferred_element_type=F32).astype(BF16)
    ref[(whole + 1) * rows :, :] = hidden[(whole + 1) * rows :, :]


def first_kernel(mine, picks, down, out, slots):
    slot_rows(mine, picks, slots)
    piece = out.shape[1] // BASE
    for q in range(BASE):
        at = slice(q * piece, (q + 1) * piece)
        out[:, at] = jnp.dot(slots[...], down[0, :, at], preferred_element_type=F32)


def down_kernel(count, theirs, picks, begun, other, *refs):
    outs, out_half, own = refs[:count], refs[count], refs[count + 1]
    slots, scratch, *spares = refs[count + 2 :]
    width = begun.shape[1]
    half, piece = width // 2, width // BASE
    rows = own.shape[0]
    here = pl.multiple_of(lax.axis_index("tensor") * half, 128)
    slot_rows(theirs, picks, slots)
    for q in range(BASE):
        at = slice(q * piece, (q + 1) * piece)
        y = begun[:, at] + jnp.dot(slots[...], other[0, :, at], preferred_element_type=F32)
        scratch[:rows, at] = y[:rows]
        scratch[rows:, at] = y[(count + 1) * rows :]
        for i in range(count):
            row = (i + 1) * rows
            outs[i][:, at] = y[row : row + BASE].astype(BF16)
            spares[i][q : q + 1, :] = y[row + BASE : row + CAP]
    own[...] = scratch[:rows, pl.ds(here, half)]
    out_half[...] = scratch[rows:, pl.ds(here, half)].astype(BF16)
    for out, spare in zip(outs, spares):
        out[:, width:] = spare[...].astype(BF16)


def mix_kernel(count, weights, coefs, own, *refs):
    back = refs[:count]
    keep, give, stack, total, *spreads = refs[count:]
    rows, half = own.shape
    core = lax.axis_index("tensor")
    here = pl.multiple_of(core * half, 128)
    there = pl.multiple_of((1 - core) * half, 128)
    for i, (block, spread) in enumerate(zip(back, spreads)):
        stack[i * rows : (i + 1) * rows, :] = unpack(block, spread)
    mixed = jnp.dot(coefs[...], stack[...], preferred_element_type=F32)
    total[...] = mixed[:rows] + mixed[rows:]
    keep[...] = total[:, pl.ds(here, half)] + weights[:, 0:1] * own[...]
    give[...] = total[:, pl.ds(there, half)]


def last_kernel(weights, keep, got, back_half, out):
    total = keep[...] + got[...] + weights[:, 1:2] * back_half[...].astype(F32)
    out[...] = total.astype(BF16)


def layer(tokens, routes, logits, gate, up, down):
    rows, width = tokens.shape
    devices = lax.axis_size("expert")
    segments = devices // logits.shape[1]
    plan, whole, last = partner_plan(devices)
    count = len(plan)
    half, hidden = width // 2, gate.shape[2]
    bf16, f32 = jnp.bfloat16, jnp.float32
    S = jax.ShapeDtypeStruct
    slots = S((BASE, width * CAP // BASE), bf16)
    spare, spread = pltpu.VMEM((BASE, width // BASE), f32), pltpu.VMEM((rows, width), f32)
    hint = pl.CostEstimate(flops=4_000_000_000, bytes_accessed=20 * MIB, transcendentals=0)
    before = call(earlier_kernel, 0, S((rows, rows), bf16), 1 * MIB, cost=hint)()
    packed = call(
        functools.partial(pack_kernel, plan[whole:], segments), 3, [slots] * (count - whole),
        2 * MIB + count * MIB // 4, [spare],
    )(tokens, routes.T, before)
    mine = []
    for j, offsets in enumerate([*plan, (last, last)]):
        x = packed[j - whole] if whole <= j < count else tokens
        mine.append(exchange(x, devices, offsets))
    mine, near = mine[:-1], mine[-1]
    other = swap_cores(down)
    hint = pl.CostEstimate(flops=4_000_000_000, bytes_accessed=20 * MIB, transcendentals=0)
    numbers = call(
        functools.partial(number_kernel, logits.shape[1]), 1, S((2, rows), jnp.int32), 1 * MIB, cost=hint
    )(routes.T)
    routed = []
    for offsets in plan[:whole]:
        routed.append(exchange(numbers, devices, offsets))
    weights, coefs = call(
        functools.partial(route_kernel, [(0, 0), (last, last)], plan, segments), 2,
        [S((rows, 128), f32), S((2 * rows, count * rows), bf16)], 1 * MIB,
    )(routes, logits)
    picks = call(functools.partial(select_kernel, segments), whole, S((whole * rows, rows), bf16), 1 * MIB)(*routed)
    theirs = []
    for m in mine:
        theirs.append(swap_cores(m))
    total, cut = (2 * count + 2) * rows, (count + 2) * rows
    keep, give = call(
        functools.partial(hidden_kernel, count), 2 * count + 4,
        [S((cut, hidden), bf16)] * 2, 12 * MIB + 8 * total * width,
        [pltpu.VMEM((total, width), bf16)] + [spread] * (2 * (count - whole)),
    )(tokens, *mine, near, *theirs, gate, up)
    got = swap_cores(give)
    begun = call(
        first_kernel, 3, S((cut, width), f32), 8 * MIB,
        [pltpu.VMEM((cut, hidden), bf16)],
    )(keep, picks, down)
    *outs, out_half, own = call(
        functools.partial(down_kernel, count), 4,
        [slots] * count + [S((rows, half), bf16), S((rows, half), f32)], 14 * MIB,
        [pltpu.VMEM((cut, hidden), bf16), pltpu.VMEM((2 * rows, width), f32)] + [spare] * count,
    )(got, picks, begun, other)
    back = []
    for o, offsets in zip([*outs, out_half], [*plan, (last, last)]):
        back.append(exchange(o, devices, offsets))
    back, back_half = back[:-1], back[-1]
    keep, give = call(
        functools.partial(mix_kernel, count), count + 3, [S((rows, half), f32)] * 2,
        4 * MIB + count * MIB,
        [pltpu.VMEM((count * rows, width), bf16), spread] + [spread] * count,
    )(weights, coefs, own, *back)
    got = swap_cores(give)
    return call(last_kernel, 4, S((rows, half), bf16), 4 * MIB)(weights, keep, got, back_half)


def solution(mesh):
    step = jax.shard_map(
        layer,
        mesh=mesh,
        in_specs=(
            P(("groups", "expert"), None),
            P(("groups", "expert"), None),
            P(("groups", "expert"), None),
            P("expert", None, "tensor"),
            P("expert", None, "tensor"),
            P("expert", "tensor", None),
        ),
        out_specs=P(("groups", "expert"), "tensor"),
        check_vma=False,
    )
    _, _, _ = partner_plan(mesh.shape["expert"])
    return step
```

```python
import functools

import jax
import jax.numpy as jnp
from jax import lax
from jax.experimental import pallas as pl
from jax.experimental.pallas import tpu as pltpu
from jax.sharding import PartitionSpec as P


CAP = 5
BASE = 4
AXES = ("expert", "tensor")
VMEM = pl.BlockSpec(memory_space=pltpu.VMEM)
MIB = 1 << 20
F32, BF16 = jnp.float32, jnp.bfloat16


def partner_plan(devices):
    if devices == 8:
        return [(2, 6), (5, 4), (3, 7)], 1, 1
    last, *rest = range(1, devices)
    half = len(rest) // 2
    return list(zip(rest[:half], rest[half:])), half // 3, last


def exchange(x, devices, offsets):
    pairs = [
        (d * 2 + c, (d ^ offsets[c]) * 2 + c) for d in range(devices) for c in range(2)
    ]
    return lax.ppermute(x, AXES, pairs)


def swap_cores(x):
    return lax.ppermute(x, "tensor", [(0, 1), (1, 0)])


def call(kernel, inputs, outs, limit, scratch=(), cost=None):
    return pl.pallas_call(
        kernel,
        out_shape=outs,
        in_specs=[VMEM] * inputs,
        out_specs=jax.tree.map(lambda _: VMEM, outs),
        scratch_shapes=scratch,
        compiler_params=pltpu.CompilerParams(vmem_limit_bytes=limit),
        cost_estimate=cost,
    )


def expert_at(offsets, segments):
    me, core = lax.axis_index("expert"), lax.axis_index("tensor")
    return (me ^ jnp.where(core == 0, offsets[0], offsets[1])) // segments


def unpack(ref, scratch):
    width = scratch.shape[1]
    piece = width // BASE
    scratch[BASE:, :] = jnp.zeros((scratch.shape[0] - BASE, width), F32)
    scratch[:BASE, :] = ref[:, :width].astype(F32)
    beside = ref[:, width:].astype(F32)
    for q in range(BASE):
        scratch[BASE:CAP, q * piece : (q + 1) * piece] = beside[q : q + 1]
    return scratch[...].astype(BF16)


def pack(rows, first, width, ref, spare):
    piece = width // BASE
    ref[:, first : first + rows.shape[1]] = rows[:BASE].astype(BF16)
    for q in range(BASE):
        at = q * piece - first
        if 0 <= at < rows.shape[1]:
            spare[q : q + 1, :] = rows[BASE:CAP, at : at + piece]


def earlier_kernel(out):
    row, column = (lax.broadcasted_iota(jnp.int32, out.shape, d) for d in range(2))
    out[...] = jnp.where(row < column, 1.0, 0.0).astype(BF16)


def pack_kernel(packed, segments, tokens, routes, before, *refs):
    outs, spare = refs[:-1], refs[-1]
    rows, width = tokens.shape
    shape = (len(packed) * rows, rows)
    row = lax.broadcasted_iota(jnp.int32, shape, 0)
    expert = jnp.zeros(shape, jnp.int32)
    for i, offsets in enumerate(packed):
        expert = jnp.where(row // rows == i, expert_at(offsets, segments), expert)
    named = (routes[0:1, :] == expert) | (routes[1:2, :] == expert)
    slot = jnp.dot(
        jnp.where(named, 1.0, 0.0).astype(BF16), before[...], preferred_element_type=F32
    )
    pick = jnp.where(named & (slot == (row % rows).astype(F32)), 1.0, 0.0).astype(BF16)
    picked = jnp.dot(pick, tokens[...], preferred_element_type=F32)
    for i, out in enumerate(outs):
        pack(picked[i * rows : (i + 1) * rows], 0, width, out, spare)
        out[:, width:] = spare[...].astype(BF16)


def number_kernel(experts, routes, out):
    rows = routes.shape[1]
    shape, square = (experts, rows), (rows, rows)
    expert = lax.broadcasted_iota(jnp.int32, shape, 0)
    hot = [jnp.where(routes[k : k + 1, :] == expert, 1.0, 0.0) for k in range(2)]
    before = lax.broadcasted_iota(jnp.int32, square, 0) < lax.broadcasted_iota(jnp.int32, square, 1)
    earlier = jnp.dot(
        (hot[0] + hot[1]).astype(BF16), jnp.where(before, 1.0, 0.0).astype(BF16), preferred_element_type=F32
    )
    for k in range(2):
        slot = jnp.sum(hot[k] * earlier, axis=0, keepdims=True)
        out[k : k + 1, :] = routes[k : k + 1, :] * rows + slot.astype(jnp.int32)


def select_kernel(segments, *refs):
    slots, out = refs[:-1], refs[-1]
    rows = out.shape[1]
    here = lax.axis_index("expert") // segments * rows
    here += lax.broadcasted_iota(jnp.int32, (rows, rows), 0)
    for i, ref in enumerate(slots):
        pick = (ref[0:1, :] == here) | (ref[1:2, :] == here)
        out[i * rows : (i + 1) * rows, :] = jnp.where(pick, 1.0, 0.0).astype(BF16)


def route_kernel(dense, packed, segments, routes_ref, logits_ref, out, coefs):
    routes, logits = routes_ref[...], logits_ref[...]
    rows = routes.shape[0]
    ids = lax.broadcasted_iota(jnp.int32, logits.shape, 1)
    picked = [
        jnp.sum(jnp.where(routes[:, k : k + 1] == ids, logits, 0.0), axis=1, keepdims=True)
        for k in range(2)
    ]
    top = jnp.maximum(picked[0], picked[1])
    raised = [jnp.exp(p - top) for p in picked]
    probs = [r / (raised[0] + raised[1]) for r in raised]

    def chosen(offsets):
        expert = expert_at(offsets, segments)
        hits = [routes[:, k : k + 1] == expert for k in range(2)]
        return hits[0] | hits[1], jnp.where(hits[0], probs[0], 0.0) + jnp.where(hits[1], probs[1], 0.0)

    lane = lax.broadcasted_iota(jnp.int32, out.shape, 1)
    total = jnp.zeros(out.shape, F32)
    for p, offsets in enumerate(dense):
        total = jnp.where(lane == p, chosen(offsets)[1], total)
    out[...] = total
    shape = (rows, coefs.shape[1])
    lane = lax.broadcasted_iota(jnp.int32, shape, 1)
    marks = jnp.zeros(shape, F32)
    value = jnp.zeros(shape, F32)
    for p, offsets in enumerate(packed):
        hit, weight = chosen(offsets)
        here = lane // rows == p
        marks = jnp.where(here & hit, 1.0, marks)
        value = jnp.where(here, weight, value)
    square = (rows, rows)
    before = lax.broadcasted_iota(jnp.int32, square, 1) < lax.broadcasted_iota(jnp.int32, square, 0)
    slot = jnp.dot(
        jnp.where(before, 1.0, 0.0).astype(BF16), marks.astype(BF16), preferred_element_type=F32
    )
    value = jnp.where((slot == (lane % rows).astype(F32)) & (marks > 0), value, 0.0)
    high = value.astype(BF16)
    coefs[:rows, :] = high
    coefs[rows:, :] = (value - high.astype(F32)).astype(BF16)


def hidden_kernel(count, *refs):
    total = 2 * count + 2
    blocks, (gate, up, keep, give, x), spreads = refs[:total], refs[total : total + 5], list(refs[total + 5 :])
    rows, _ = blocks[0].shape
    for i, block in enumerate(blocks):
        packed = block.shape[0] != rows
        x[i * rows : (i + 1) * rows, :] = unpack(block, spreads.pop()) if packed else block[...]
    g = jnp.dot(x[...], gate[0], preferred_element_type=jnp.float32)
    u = jnp.dot(x[...], up[0], preferred_element_type=jnp.float32)
    h = (g / (1.0 + jnp.exp(-g)) * u).astype(jnp.bfloat16)
    cut = (count + 2) * rows
    keep[...] = h[:cut]
    give[:rows, :] = h[:rows]
    give[rows : rows + count * rows, :] = h[cut:]
    give[rows + count * rows :, :] = h[cut - rows : cut]


def slot_rows(hidden, picks, ref):
    rows = picks.shape[1]
    whole = picks.shape[0] // rows
    ref[:rows, :] = hidden[:rows, :]
    for i in range(whole):
        at = slice((i + 1) * rows, (i + 2) * rows)
        pick = picks[i * rows : (i + 1) * rows, :]
        ref[at, :] = jnp.dot(pick, hidden[at, :], preferred_element_type=F32).astype(BF16)
    ref[(whole + 1) * rows :, :] = hidden[(whole + 1) * rows :, :]


def first_kernel(mine, picks, down, out, slots):
    slot_rows(mine, picks, slots)
    piece = out.shape[1] // BASE
    for q in range(BASE):
        at = slice(q * piece, (q + 1) * piece)
        out[:, at] = jnp.dot(slots[...], down[0, :, at], preferred_element_type=F32)


def down_kernel(count, theirs, picks, begun, other, *refs):
    outs, out_half, own = refs[:count], refs[count], refs[count + 1]
    slots, scratch, *spares = refs[count + 2 :]
    width = begun.shape[1]
    half, piece = width // 2, width // BASE
    rows = own.shape[0]
    here = pl.multiple_of(lax.axis_index("tensor") * half, 128)
    slot_rows(theirs, picks, slots)
    for q in range(BASE):
        at = slice(q * piece, (q + 1) * piece)
        y = begun[:, at] + jnp.dot(slots[...], other[0, :, at], preferred_element_type=F32)
        scratch[:rows, at] = y[:rows]
        scratch[rows:, at] = y[(count + 1) * rows :]
        for i in range(count):
            row = (i + 1) * rows
            outs[i][:, at] = y[row : row + BASE].astype(BF16)
            spares[i][q : q + 1, :] = y[row + BASE : row + CAP]
    own[...] = scratch[:rows, pl.ds(here, half)]
    out_half[...] = scratch[rows:, pl.ds(here, half)].astype(BF16)
    for out, spare in zip(outs, spares):
        out[:, width:] = spare[...].astype(BF16)


def mix_kernel(count, weights, coefs, own, *refs):
    back = refs[:count]
    keep, give, stack, total, *spreads = refs[count:]
    rows, half = own.shape
    core = lax.axis_index("tensor")
    here = pl.multiple_of(core * half, 128)
    there = pl.multiple_of((1 - core) * half, 128)
    for i, (block, spread) in enumerate(zip(back, spreads)):
        stack[i * rows : (i + 1) * rows, :] = unpack(block, spread)
    mixed = jnp.dot(coefs[...], stack[...], preferred_element_type=F32)
    total[...] = mixed[:rows] + mixed[rows:]
    keep[...] = total[:, pl.ds(here, half)] + weights[:, 0:1] * own[...]
    give[...] = total[:, pl.ds(there, half)].astype(BF16)


def last_kernel(weights, keep, got, back_half, out):
    total = keep[...] + got[...].astype(F32) + weights[:, 1:2] * back_half[...].astype(F32)
    out[...] = total.astype(BF16)


def layer(tokens, routes, logits, gate, up, down):
    rows, width = tokens.shape
    devices = lax.axis_size("expert")
    segments = devices // logits.shape[1]
    plan, whole, last = partner_plan(devices)
    count = len(plan)
    half, hidden = width // 2, gate.shape[2]
    bf16, f32 = jnp.bfloat16, jnp.float32
    S = jax.ShapeDtypeStruct
    slots = S((BASE, width * CAP // BASE), bf16)
    spare, spread = pltpu.VMEM((BASE, width // BASE), f32), pltpu.VMEM((rows, width), f32)
    hint = pl.CostEstimate(flops=4_000_000_000, bytes_accessed=20 * MIB, transcendentals=0)
    before = call(earlier_kernel, 0, S((rows, rows), bf16), 1 * MIB, cost=hint)()
    packed = call(
        functools.partial(pack_kernel, plan[whole:], segments), 3, [slots] * (count - whole),
        2 * MIB + count * MIB // 4, [spare],
    )(tokens, routes.T, before)
    mine = []
    for j, offsets in enumerate([*plan, (last, last)]):
        x = packed[j - whole] if whole <= j < count else tokens
        mine.append(exchange(x, devices, offsets))
    mine, near = mine[:-1], mine[-1]
    other = swap_cores(down)
    hint = pl.CostEstimate(flops=4_000_000_000, bytes_accessed=20 * MIB, transcendentals=0)
    numbers = call(
        functools.partial(number_kernel, logits.shape[1]), 1, S((2, rows), jnp.int32), 1 * MIB, cost=hint
    )(routes.T)
    routed = []
    for offsets in plan[:whole]:
        routed.append(exchange(numbers, devices, offsets))
    weights, coefs = call(
        functools.partial(route_kernel, [(0, 0), (last, last)], plan, segments), 2,
        [S((rows, 128), f32), S((2 * rows, count * rows), bf16)], 1 * MIB,
    )(routes, logits)
    picks = call(functools.partial(select_kernel, segments), whole, S((whole * rows, rows), bf16), 1 * MIB)(*routed)
    theirs = []
    for m in mine:
        theirs.append(swap_cores(m))
    total, cut = (2 * count + 2) * rows, (count + 2) * rows
    keep, give = call(
        functools.partial(hidden_kernel, count), 2 * count + 4,
        [S((cut, hidden), bf16)] * 2, 12 * MIB + 8 * total * width,
        [pltpu.VMEM((total, width), bf16)] + [spread] * (2 * (count - whole)),
    )(tokens, *mine, near, *theirs, gate, up)
    got = swap_cores(give)
    begun = call(
        first_kernel, 3, S((cut, width), f32), 8 * MIB,
        [pltpu.VMEM((cut, hidden), bf16)],
    )(keep, picks, down)
    *outs, out_half, own = call(
        functools.partial(down_kernel, count), 4,
        [slots] * count + [S((rows, half), bf16), S((rows, half), f32)], 14 * MIB,
        [pltpu.VMEM((cut, hidden), bf16), pltpu.VMEM((2 * rows, width), f32)] + [spare] * count,
    )(got, picks, begun, other)
    back = []
    for o, offsets in zip([*outs, out_half], [*plan, (last, last)]):
        back.append(exchange(o, devices, offsets))
    back, back_half = back[:-1], back[-1]
    keep, give = call(
        functools.partial(mix_kernel, count), count + 3, [S((rows, half), f32), S((rows, half), bf16)],
        4 * MIB + count * MIB,
        [pltpu.VMEM((count * rows, width), bf16), spread] + [spread] * count,
    )(weights, coefs, own, *back)
    got = swap_cores(give)
    return call(last_kernel, 4, S((rows, half), bf16), 4 * MIB)(weights, keep, got, back_half)


def solution(mesh):
    step = jax.shard_map(
        layer,
        mesh=mesh,
        in_specs=(
            P(("groups", "expert"), None),
            P(("groups", "expert"), None),
            P(("groups", "expert"), None),
            P("expert", None, "tensor"),
            P("expert", None, "tensor"),
            P("expert", "tensor", None),
        ),
        out_specs=P(("groups", "expert"), "tensor"),
        check_vma=False,
    )
    _, _, _ = partner_plan(mesh.shape["expert"])
    return step
```
